32 devices in a mesh: seq: 2 (over x), dp: 4 (over y, core), tp: 4 (over z).
Axes of the slice: x: 2, y: 2, z: 4, core: 2. Of those that a mesh axis runs over, the one named last changes fastest.
Arguments:
- patches: bfloat16 [16, 384, 1152], P(('dp', 'tp'), 'seq'), parts along dimension 0, may hold values from -6 to 6
- seg_ids: int32 [16, 384], P(('dp', 'tp'), 'seq'), parts along dimension 0, may hold values from 0 to 11, never falling along the last dimension, each value on 1 to 96 neighbouring positions
- pos_rows: int32 [16, 384], P(('dp', 'tp'), 'seq'), parts along dimension 0, may hold values from 0 to 63
- pos_cols: int32 [16, 384], P(('dp', 'tp'), 'seq'), parts along dimension 0, may hold values from 0 to 63
- row_table: bfloat16 [64, 1152], replicated, may hold values from -3 to 3
- col_table: bfloat16 [64, 1152], replicated, may hold values from -3 to 3
- ln1_gain: float32 [1152], replicated, may hold values from 0.5 to 1.5
- ln1_bias: float32 [1152], replicated, may hold values from -1.75 to 1.75
- w_qkv: bfloat16 [1152, 3456], P(None, 'seq'), may hold values from -0.41247896 to 0.41247896
- w_out: bfloat16 [1152, 1152], P('seq'), may hold values from -0.1875 to 0.1875
- out_bias: bfloat16 [1152], replicated, may hold values from -3 to 3
- ln2_gain: float32 [1152], replicated, may hold values from 0.5 to 1.5
- ln2_bias: float32 [1152], replicated, may hold values from -1.75 to 1.75
- w_fc1: bfloat16 [1152, 4304], P(None, 'tp'), may hold values from -0.1875 to 0.1875
- fc1_bias: bfloat16 [4304], P('tp'), may hold values from -3 to 3
- w_fc2: bfloat16 [4304, 1152], P('tp'), may hold values from -0.09375 to 0.09375
- fc2_bias: bfloat16 [1152], replicated, may hold values from -3 to 3
Outputs:
- encoded: bfloat16 [16, 384, 1152], P(('dp', 'tp'), 'seq'), parts along dimension 0
The draws below stay inside these ranges and needn't reach their ends.
There are 4 independent parts, one for each index of `dp`. The reference program is written for one: setup_inputs(seed, part) draws one part's arguments, and reference() takes and returns one part's arrays. A program takes and returns all parts, laid end to end along the dimension named above; an argument that names none is the same for every part. Nothing has to cross between parts.
Inputs may be any that keep to these rules, and one draw needn't show every extreme that they name: `seg_ids`: image numbers never fall along a sequence; every image has 1 to 96 tokens.
All inputs are finite; a program needn't handle non-finite values.
Results may differ from the reference program's by a relative error of at most 0.0095.
Values may be sent and summed in bfloat16 or wider, within the bound.
No kernel may reach another device: no remote copies, remote signals or barrier semaphores. Data moves between devices by JAX's collectives and lax.ppermute only.
A program may use at most 64 MiB of HBM per device.

```python
import math
import jax
import jax.numpy as jnp
import numpy as np
from jax import lax

D = 1152
HEADS = 16
FF = 4304
GRID = 64
IMAGES = 12
HEAD_DIM = 72
LENGTH = 384
NSEQ = 4
MOST = 96


def draw_w_qkv(key, part):
    head_dim = D // HEADS
    shape = (D, HEADS, 3, head_dim)
    weights = jnp.clip(jax.random.normal(key, shape, jnp.float32), -6.0, 6.0) / jnp.sqrt(float(D))
    return weights.reshape(D, HEADS * 3 * head_dim).astype(jnp.bfloat16)


def touch_ends(result, rng, smallest, top_value):
    longest = result.shape.index(max(result.shape))
    spots = []
    for shift in (0, 1):
        where = [jax.random.randint(jax.random.fold_in(rng, axis), (), 0, length) for axis, length in enumerate(result.shape)]
        where[longest] = (where[longest] + shift) % result.shape[longest]
        spots.append(tuple(where))
    return result.at[spots[0]].set(smallest).at[spots[1]].set(top_value)


def steps_of(rng, shape, shards, least, top_value):
    level = 1.0
    for dim, blocks in shards:
        heights = jax.random.uniform(jax.random.fold_in(jax.random.fold_in(rng, 6), dim), (blocks,), jnp.float32, least / len(shards), top_value / len(shards))
        level = level * jnp.repeat(jnp.exp(heights), shape[dim] // blocks).reshape((-1,) + (1,) * (len(shape) - 1 - dim))
    return level


def length_profile(number_of, total, reach, slope):
    weights = [(1 << 20) // math.isqrt(standing ** slope) + 1 for standing in range(2, number_of + 1)]
    surplus, holding = total - reach - (number_of - 1), [1] * (number_of - 1)
    while surplus > 0:
        movable = [i for i in range(number_of - 1) if holding[i] < reach]
        mass, budget = sum([weights[i] for i in movable]), surplus
        for i in movable:
            addition = min(reach - holding[i], max(1, budget * weights[i] // mass), surplus)
            holding[i] = holding[i] + addition
            surplus = surplus - addition
    return np.array([reach] + holding)


def ragged(own_key, number_of, total, most, lean):
    if number_of == 2:
        one = jax.random.randint(own_key, (), max(1, total - most), min(most, total - 1) + 1)
        return jnp.stack([one, total - one])
    tallies = jnp.asarray(length_profile(number_of, total, most, lean), jnp.int32)
    couples = (number_of - 1) // 2
    donor, taker = tallies[1:1 + 2 * couples:2], tallies[2:2 + 2 * couples:2]
    slack = jnp.minimum(donor - 1, most - taker)
    shifted = jax.random.randint(jax.random.fold_in(own_key, 1), (couples,), 0, 1 << 20) % (slack + 1)
    tallies = tallies.at[1:1 + 2 * couples:2].set(donor - shifted).at[2:2 + 2 * couples:2].set(taker + shifted)
    return tallies[jax.random.permutation(jax.random.fold_in(own_key, 2), number_of)]


def scatter_about(key, dims, scale, most, pieces=(), dtype=jnp.bfloat16):
    factor_of = steps_of(key, dims, pieces, -0.22, 0.18) if pieces else 1.0
    drawn = jax.random.normal(key, dims, jnp.float32) * scale * factor_of
    return jnp.minimum(jnp.maximum(drawn, -most), most).astype(dtype)


def setup_inputs(seed: int = 0, part: int = 0) -> dict:
    seeds = jax.random.split(jax.random.key(seed), 18)
    part_keys = jax.random.split(jax.random.fold_in(seeds[17], part), 18)
    return {
        "patches": scatter_about(part_keys[0], (NSEQ, LENGTH, D), 1.0, 6.0, ((0, 4), (1, 2))),
        "seg_ids": jax.vmap(lambda own: jnp.searchsorted(jnp.cumsum(ragged(own, IMAGES, LENGTH, MOST, 1)), jnp.arange(LENGTH), side="right"))(jax.random.split(part_keys[1], NSEQ)).reshape((NSEQ, LENGTH)).astype(jnp.int32),
        "pos_rows": touch_ends(jax.random.randint(part_keys[2], (NSEQ, LENGTH), 0, GRID), jax.random.fold_in(part_keys[2], 1), 0, GRID - 1).astype(jnp.int32),
        "pos_cols": touch_ends(jax.random.randint(part_keys[3], (NSEQ, LENGTH), 0, GRID), jax.random.fold_in(part_keys[3], 1), 0, GRID - 1).astype(jnp.int32),
        "row_table": scatter_about(seeds[4], (GRID, D), 0.5, 3.0),
        "col_table": scatter_about(seeds[5], (GRID, D), 0.5, 3.0),
        "ln1_gain": jnp.clip(1.0 + 0.1 * jax.random.normal(seeds[6], (D,), jnp.float32), 0.5, 1.5),
        "ln1_bias": scatter_about(seeds[7], (D,), 0.3, 1.75, (), jnp.float32),
        "w_qkv": draw_w_qkv(jax.random.fold_in(seeds[17], 71), part),
        "w_out": scatter_about(seeds[9], (D, D), D ** -0.5, 0.1875, ((0, 2),)),
        "out_bias": scatter_about(seeds[10], (D,), 0.5, 3.0),
        "ln2_gain": jnp.clip(1.0 + 0.1 * jax.random.normal(seeds[11], (D,), jnp.float32), 0.5, 1.5),
        "ln2_bias": scatter_about(seeds[12], (D,), 0.3, 1.75, (), jnp.float32),
        "w_fc1": scatter_about(seeds[13], (D, FF), D ** -0.5, 0.1875, ((1, 4),)),
        "fc1_bias": scatter_about(seeds[14], (FF,), 0.5, 3.0, ((0, 4),)),
        "w_fc2": scatter_about(seeds[15], (FF, D), FF ** -0.5, 0.09375, ((0, 4),)),
        "fc2_bias": scatter_about(seeds[16], (D,), 0.5, 3.0),
    }


def layer_norm(values, gain, shift):
    center = lax.optimization_barrier(jnp.mean(values, -1, keepdims=True))
    spread = lax.optimization_barrier(jnp.mean(jnp.square(values - center), -1, keepdims=True))
    return (values - center) * lax.rsqrt(spread + 1e-06) * gain + shift

def attend_one(item, segments):
    query = item[:, 0]
    keys = item[:, 1]
    value = item[:, 2]
    scores = jnp.dot(query, keys.T, preferred_element_type=jnp.float32) / math.sqrt(query.shape[-1])
    same = segments[:, None] == segments[None, :]
    scores = jnp.where(same, scores, -jnp.inf)
    top = lax.optimization_barrier(jnp.max(scores, -1, keepdims=True))
    expo = jnp.exp(scores - top)
    probs = (expo / lax.optimization_barrier(jnp.sum(expo, -1, keepdims=True))).astype(jnp.bfloat16)
    return jnp.dot(probs, value, preferred_element_type=jnp.float32).astype(jnp.bfloat16)

def reference(patches, seg_ids, pos_rows, pos_cols, row_table, col_table, ln1_gain, ln1_bias, w_qkv, w_out, out_bias, ln2_gain, ln2_bias, w_fc1, fc1_bias, w_fc2, fc2_bias):
    embedded = patches.astype(jnp.float32) + row_table[pos_rows].astype(jnp.float32) + col_table[pos_cols].astype(jnp.float32)
    embedded = embedded.reshape(NSEQ * LENGTH, D)
    normed = layer_norm(embedded, ln1_gain, ln1_bias).astype(jnp.bfloat16)
    qkv = jnp.dot(normed, w_qkv, preferred_element_type=jnp.float32).astype(jnp.bfloat16)
    qkv = qkv.reshape(NSEQ, LENGTH, HEADS, 3, HEAD_DIM).transpose(0, 2, 1, 3, 4)
    qkv = qkv.reshape(NSEQ * HEADS, LENGTH, 3, HEAD_DIM)
    segments = jnp.repeat(seg_ids, HEADS, axis=0)
    mixed = lax.map(lambda pair: attend_one(pair[0], pair[1]), (qkv, segments))
    mixed = mixed.reshape(NSEQ, HEADS, LENGTH, HEAD_DIM).transpose(0, 2, 1, 3).reshape(NSEQ * LENGTH, D)
    attended = embedded + jnp.dot(mixed, w_out, preferred_element_type=jnp.float32) + out_bias.astype(jnp.float32)
    normed2 = layer_norm(attended, ln2_gain, ln2_bias).astype(jnp.bfloat16)
    hidden = jax.nn.gelu(jnp.dot(normed2, w_fc1, preferred_element_type=jnp.float32) + fc1_bias.astype(jnp.float32), approximate=True).astype(jnp.bfloat16)
    reduced = jnp.dot(hidden, w_fc2, preferred_element_type=jnp.float32)
    encoded = (attended + reduced + fc2_bias.astype(jnp.float32)).astype(jnp.bfloat16)
    return encoded.reshape(NSEQ, LENGTH, D)
```

```python
import math

import jax
import jax.numpy as jnp
from jax import lax
from jax.sharding import PartitionSpec as P

HEADS = 16


def layer_norm(values, gain, shift):
    center = jnp.mean(values, -1, keepdims=True)
    spread = jnp.mean(jnp.square(values - center), -1, keepdims=True)
    return (values - center) * lax.rsqrt(spread + 1e-06) * gain + shift


def attend_head(item, segments):
    length = item.shape[0]
    head_dim = item.shape[1] // 3
    block = min(512, length)
    query = item[:, :head_dim].reshape(length // block, block, head_dim)
    seg_query = segments.reshape(length // block, block)
    keys = item[:, head_dim : 2 * head_dim]
    value = item[:, 2 * head_dim :]

    def one_block(pair):
        rows, seg_rows = pair
        scores = lax.dot_general(
            rows, keys, (((1,), (1,)), ((), ())), preferred_element_type=jnp.float32
        ) / math.sqrt(head_dim)
        same = seg_rows[:, None] == segments[None, :]
        scores = jnp.where(same, scores, -jnp.inf)
        top = jnp.max(scores, -1, keepdims=True)
        expo = jnp.exp(scores - top)
        probs = (expo / jnp.sum(expo, -1, keepdims=True)).astype(jnp.bfloat16)
        return jnp.dot(probs, value, preferred_element_type=jnp.float32).astype(jnp.bfloat16)

    return lax.map(one_block, (query, seg_query)).reshape(length, head_dim)


def gathered_layer(
    patches,
    seg_ids,
    pos_rows,
    pos_cols,
    row_table,
    col_table,
    ln1_gain,
    ln1_bias,
    w_qkv,
    w_out,
    out_bias,
    ln2_gain,
    ln2_bias,
    w_fc1,
    fc1_bias,
    w_fc2,
    fc2_bias,
):
    width = patches.shape[2]
    head_dim = width // HEADS
    heads_here = w_qkv.shape[1] // (3 * head_dim)
    levels = jnp.arange(row_table.shape[0], dtype=jnp.int32)
    row_hot = (pos_rows[0][:, None] == levels[None, :]).astype(jnp.bfloat16)
    col_hot = (pos_cols[0][:, None] == levels[None, :]).astype(jnp.bfloat16)
    embedded = patches[0].astype(jnp.float32) + jnp.dot(
        row_hot, row_table, preferred_element_type=jnp.float32
    )
    embedded = embedded + jnp.dot(col_hot, col_table, preferred_element_type=jnp.float32)
    normed = layer_norm(embedded, ln1_gain, ln1_bias).astype(jnp.bfloat16)
    seg_all = lax.all_gather(seg_ids[0], "seq", axis=0, tiled=True)
    qkv = jnp.dot(
        lax.all_gather(normed, "seq", axis=0, tiled=True), w_qkv, preferred_element_type=jnp.float32
    ).astype(jnp.bfloat16)
    mixed = jax.vmap(attend_head, in_axes=(1, None), out_axes=1)(
        qkv.reshape(qkv.shape[0], heads_here, 3 * head_dim), seg_all
    )
    mixed = mixed.reshape(mixed.shape[0], heads_here * head_dim)
    rows = mixed
    projected = lax.psum_scatter(
        jnp.dot(rows, w_out, preferred_element_type=jnp.float32).astype(jnp.bfloat16),
        "seq",
        scatter_dimension=0,
        tiled=True,
    ).astype(jnp.float32)
    attended = embedded + projected + out_bias.astype(jnp.float32)
    normed2 = layer_norm(attended, ln2_gain, ln2_bias).astype(jnp.bfloat16)
    inner = jnp.dot(
        lax.all_gather(normed2, "tp", axis=0, tiled=True), w_fc1, preferred_element_type=jnp.float32
    ) + fc1_bias.astype(jnp.float32)
    hidden = jax.nn.gelu(inner, approximate=True).astype(jnp.bfloat16)
    rows = hidden
    reduced = lax.psum_scatter(
        jnp.dot(rows, w_fc2, preferred_element_type=jnp.float32).astype(jnp.bfloat16),
        "tp",
        scatter_dimension=0,
        tiled=True,
    ).astype(jnp.float32)
    encoded = (attended + reduced + fc2_bias.astype(jnp.float32)).astype(jnp.bfloat16)
    return encoded[None]


def after(value, *earlier):
    return lax.optimization_barrier((value,) + earlier)[0]


def swap(values, axis, size, bit):
    return lax.ppermute(values, axis, [(i, i ^ bit) for i in range(size)])


def wide_dot(left, right):
    return jnp.dot(left, right, preferred_element_type=jnp.float32)


def dot_t(left, right):
    return lax.dot_general(
        left, right, (((1,), (1,)), ((), ())), preferred_element_type=jnp.float32
    )


def swapped_layer(sizes):
    seq, dp, tp = sizes

    def per_device(
        patches,
        seg_ids,
        pos_rows,
        pos_cols,
        row_table,
        col_table,
        ln1_gain,
        ln1_bias,
        w_qkv,
        w_out,
        out_bias,
        ln2_gain,
        ln2_bias,
        w_fc1,
        fc1_bias,
        w_fc2,
        fc2_bias,
    ):
        tokens, width = patches.shape[1:]
        head_dim = width // HEADS
        heads_here = w_qkv.shape[1] // (3 * head_dim)
        hidden = w_fc2.shape[0]
        side = lax.axis_index("seq")
        place = side * dp + lax.axis_index("dp")
        holders = seq * dp
        rows = -(-hidden // (8 * holders)) * 8
        overlap = rows * holders - hidden
        begin = jnp.minimum(place * rows, hidden - rows)
        fc1_rows = w_fc1.T
        share1 = lax.dynamic_slice(fc1_rows, (begin, 0), (rows, width))
        share2 = lax.dynamic_slice(w_fc2, (begin, 0), (rows, width))
        repeated = (place == holders - 1) & (jnp.arange(rows) < overlap)
        share2 = jnp.where(repeated[:, None], jnp.zeros_like(share2), share2)
        far1 = swap(share1, "tp", tp, 2)
        far2 = swap(share2, "tp", tp, 2)
        far_bias = swap(fc1_bias, "tp", tp, 2)

        levels = jnp.arange(row_table.shape[0], dtype=jnp.int32)
        row_hot = (pos_rows[0][:, None] == levels[None, :]).astype(jnp.bfloat16)
        col_hot = (pos_cols[0][:, None] == levels[None, :]).astype(jnp.bfloat16)
        embedded = patches[0].astype(jnp.float32) + wide_dot(row_hot, row_table)
        embedded = embedded + wide_dot(col_hot, col_table)
        normed = layer_norm(embedded, ln1_gain, ln1_bias).astype(jnp.bfloat16)
        normed_other = swap(normed, "seq", seq, 1)
        seg_other = swap(seg_ids[0], "seq", seq, 1)
        qkv_rows = w_qkv.T
        qkv_own = dot_t(normed, qkv_rows).astype(jnp.bfloat16)
        qkv_other = dot_t(normed_other, qkv_rows).astype(jnp.bfloat16)
        qkv = jnp.concatenate([qkv_own, qkv_other])
        seg_all = jnp.concatenate([seg_ids[0], seg_other])

        def spread(share):
            along_x = swap(share, "seq", seq, 1)
            along_y = swap(share, "dp", dp, 2)
            both = lax.ppermute(
                share, ("seq", "dp"), [(i, i ^ (dp + 2)) for i in range(seq * dp)]
            )
            near = jnp.concatenate([share, along_x, along_y, both])
            return near

        near1 = spread(after(far1, qkv_other))
        mixed = jax.vmap(attend_head, in_axes=(1, None), out_axes=1)(
            qkv.reshape(2 * tokens, heads_here, 3 * head_dim), seg_all
        )
        mixed = mixed.reshape(2 * tokens, heads_here * head_dim)
        sent = wide_dot(mixed[tokens:], w_out).astype(jnp.bfloat16)
        got = swap(sent, "seq", seq, 1)
        kept = wide_dot(mixed[:tokens], w_out)
        cross1 = swap(after(near1, sent), "dp", dp, 1)
        near2 = spread(after(far2, near1))
        attended = embedded + (kept + got.astype(jnp.float32)) + out_bias.astype(jnp.float32)
        normed2 = layer_norm(attended, ln2_gain, ln2_bias).astype(jnp.bfloat16)
        partner = swap(normed2, "tp", tp, 1)
        cross2 = swap(near2, "dp", dp, 1)

        starts = jnp.minimum(jnp.arange(holders) * rows, hidden - rows)
        order = []
        for core in (0, 1):
            for step in (0, dp, 2, dp + 2):
                order.append(step ^ core)
        chosen = jnp.take(starts, place ^ jnp.array(order))
        picks = (chosen[:, None] + jnp.arange(rows)[None, :]).reshape(-1)
        bias_far = jnp.take(far_bias, picks).astype(jnp.float32)
        bias_here = fc1_bias.astype(jnp.float32)

        def mlp(inputs):
            here = jax.nn.gelu(dot_t(inputs, fc1_rows) + bias_here, approximate=True)
            total = wide_dot(here.astype(jnp.bfloat16), w_fc2)
            half = 4 * rows
            for up, bias, down in (
                (near1, bias_far[:half], near2),
                (cross1, bias_far[half:], cross2),
            ):
                there = jax.nn.gelu(dot_t(inputs, up) + bias, approximate=True)
                total = total + wide_dot(there.astype(jnp.bfloat16), down)
            return total

        back = swap(mlp(partner).astype(jnp.bfloat16), "tp", tp, 1)
        encoded = attended + (mlp(normed2) + back.astype(jnp.float32))
        return (encoded + fc2_bias.astype(jnp.float32)).astype(jnp.bfloat16)[None]

    return per_device


def solution(mesh):
    placed = (
        P(("dp", "tp"), "seq", None),
        P(("dp", "tp"), "seq"),
        P(("dp", "tp"), "seq"),
        P(("dp", "tp"), "seq"),
        P(),
        P(),
        P(),
        P(),
        P(None, "seq"),
        P("seq", None),
        P(),
        P(),
        P(),
        P(None, "tp"),
        P("tp"),
        P("tp", None),
        P(),
    )
    sizes = mesh.shape["seq"], mesh.shape["dp"], mesh.shape["tp"]
    layer = swapped_layer(sizes) if sizes == (2, 4, 4) else gathered_layer
    return jax.shard_map(
        layer,
        mesh=mesh,
        in_specs=placed,
        out_specs=P(("dp", "tp"), "seq", None),
        check_vma=False,
    )
```

```python
import functools
import math

import jax
import jax.numpy as jnp
from jax import lax
from jax.experimental import pallas as pl
from jax.experimental.pallas import tpu as pltpu
from jax.sharding import PartitionSpec as P


HEADS = 16


def layer_norm(values, gain, shift):
    center = jnp.mean(values, -1, keepdims=True)
    spread = jnp.mean(jnp.square(values - center), -1, keepdims=True)
    return (values - center) * lax.rsqrt(spread + 1e-06) * gain + shift


def attend_head(item, segments):
    length = item.shape[0]
    head_dim = item.shape[1] // 3
    block = min(512, length)
    query = item[:, :head_dim].reshape(length // block, block, head_dim)
    seg_query = segments.reshape(length // block, block)
    keys = item[:, head_dim : 2 * head_dim]
    value = item[:, 2 * head_dim :]

    def one_block(pair):
        rows, seg_rows = pair
        scores = lax.dot_general(
            rows, keys, (((1,), (1,)), ((), ())), preferred_element_type=jnp.float32
        ) / math.sqrt(head_dim)
        same = seg_rows[:, None] == segments[None, :]
        scores = jnp.where(same, scores, -jnp.inf)
        top = jnp.max(scores, -1, keepdims=True)
        expo = jnp.exp(scores - top)
        probs = (expo / jnp.sum(expo, -1, keepdims=True)).astype(jnp.bfloat16)
        return jnp.dot(probs, value, preferred_element_type=jnp.float32).astype(jnp.bfloat16)

    return lax.map(one_block, (query, seg_query)).reshape(length, head_dim)


def gathered_layer(
    patches,
    seg_ids,
    pos_rows,
    pos_cols,
    row_table,
    col_table,
    ln1_gain,
    ln1_bias,
    w_qkv,
    w_out,
    out_bias,
    ln2_gain,
    ln2_bias,
    w_fc1,
    fc1_bias,
    w_fc2,
    fc2_bias,
):
    width = patches.shape[2]
    head_dim = width // HEADS
    heads_here = w_qkv.shape[1] // (3 * head_dim)
    levels = jnp.arange(row_table.shape[0], dtype=jnp.int32)
    row_hot = (pos_rows[0][:, None] == levels[None, :]).astype(jnp.bfloat16)
    col_hot = (pos_cols[0][:, None] == levels[None, :]).astype(jnp.bfloat16)
    embedded = patches[0].astype(jnp.float32) + jnp.dot(
        row_hot, row_table, preferred_element_type=jnp.float32
    )
    embedded = embedded + jnp.dot(col_hot, col_table, preferred_element_type=jnp.float32)
    normed = layer_norm(embedded, ln1_gain, ln1_bias).astype(jnp.bfloat16)
    seg_all = lax.all_gather(seg_ids[0], "seq", axis=0, tiled=True)
    qkv = jnp.dot(
        lax.all_gather(normed, "seq", axis=0, tiled=True), w_qkv, preferred_element_type=jnp.float32
    ).astype(jnp.bfloat16)
    mixed = jax.vmap(attend_head, in_axes=(1, None), out_axes=1)(
        qkv.reshape(qkv.shape[0], heads_here, 3 * head_dim), seg_all
    )
    mixed = mixed.reshape(mixed.shape[0], heads_here * head_dim)
    rows = mixed
    projected = lax.psum_scatter(
        jnp.dot(rows, w_out, preferred_element_type=jnp.float32).astype(jnp.bfloat16),
        "seq",
        scatter_dimension=0,
        tiled=True,
    ).astype(jnp.float32)
    attended = embedded + projected + out_bias.astype(jnp.float32)
    normed2 = layer_norm(attended, ln2_gain, ln2_bias).astype(jnp.bfloat16)
    inner = jnp.dot(
        lax.all_gather(normed2, "tp", axis=0, tiled=True), w_fc1, preferred_element_type=jnp.float32
    ) + fc1_bias.astype(jnp.float32)
    hidden = jax.nn.gelu(inner, approximate=True).astype(jnp.bfloat16)
    rows = hidden
    reduced = lax.psum_scatter(
        jnp.dot(rows, w_fc2, preferred_element_type=jnp.float32).astype(jnp.bfloat16),
        "tp",
        scatter_dimension=0,
        tiled=True,
    ).astype(jnp.float32)
    encoded = (attended + reduced + fc2_bias.astype(jnp.float32)).astype(jnp.bfloat16)
    return encoded[None]


def after(value, *earlier):
    return lax.optimization_barrier((value,) + earlier)[0]


def swap(values, axis, size, bit):
    return lax.ppermute(values, axis, [(i, i ^ bit) for i in range(size)])


def wide_dot(left, right):
    return jnp.dot(left, right, preferred_element_type=jnp.float32)


def dot_t(left, right):
    return lax.dot_general(
        left, right, (((1,), (1,)), ((), ())), preferred_element_type=jnp.float32
    )


def tn_dot(left, right):
    return lax.dot_general(
        left, right, (((0,), (0,)), ((), ())), preferred_element_type=jnp.float32
    )


def norm_rows(values, gain, shift):
    center = jnp.mean(values, -1, keepdims=True)
    moved = values - center
    spread = jnp.mean(moved * moved, -1, keepdims=True)
    return moved * lax.rsqrt(spread + 1e-06) * gain + shift


def embed_kernel(patch, rows, cols, row_tab, col_tab, gain, shift, embedded, normed):
    tokens = patch.shape[0]
    grid = row_tab.shape[0]
    level = lax.broadcasted_iota(jnp.int32, (grid, tokens), 0)
    hot = jnp.concatenate([level == rows[...], level == cols[...]], 0)
    hot = jnp.where(hot, 1.0, 0.0).astype(jnp.bfloat16)
    table = jnp.concatenate([row_tab[...], col_tab[...]], 0)
    values = patch[...].astype(jnp.float32) + tn_dot(hot, table)
    embedded[...] = values
    normed[...] = norm_rows(values, gain[...][None], shift[...][None]).astype(jnp.bfloat16)


def qkv_kernel(normed, weight, out):
    head_dim = out.shape[1]
    product = dot_t(weight[...], normed[...])
    for part in range(out.shape[0]):
        out[part] = product[part * head_dim : (part + 1) * head_dim].astype(jnp.bfloat16)


def column_of(row):
    length = row.shape[1]
    across = lax.broadcasted_iota(jnp.int32, (length, length), 0)
    along = lax.broadcasted_iota(jnp.int32, (length, length), 1)
    return jnp.sum(jnp.where(across == along, row, 0.0), -1, keepdims=True)


def attend_kernel(near, far, seg_near, seg_far, weight, out, mixed):
    head_dim = near.shape[1]
    heads = near.shape[0] // 3
    scale = math.log2(math.e) / math.sqrt(head_dim)
    asked = seg_near[...].astype(jnp.float32)
    same = [column_of(seg[...].astype(jnp.float32)) == asked for seg in (seg_near, seg_far)]
    for head in range(heads):
        query = near[3 * head]
        scores = []
        for side, keep in zip((near, far), same):
            raw = tn_dot(side[3 * head + 1], query)
            scores.append(jnp.where(keep, raw, -1e30))
        top = jnp.maximum(
            jnp.max(scores[0], 0, keepdims=True), jnp.max(scores[1], 0, keepdims=True)
        )
        total = 0.0
        result = 0.0
        for side, raw in zip((near, far), scores):
            expo = jnp.exp2((raw - top) * scale)
            total = total + jnp.sum(expo, 0, keepdims=True)
            result = result + wide_dot(side[3 * head + 2], expo.astype(jnp.bfloat16))
        mixed[head * head_dim : (head + 1) * head_dim, :] = result / total
    out[...] = tn_dot(mixed[...].astype(jnp.bfloat16), weight[...]).astype(out.dtype)


def join_kernel(embedded, kept, got, bias, gain, shift, attended, normed):
    values = embedded[...] + (kept[...] + got[...].astype(jnp.float32))
    values = values + bias[...].astype(jnp.float32)[None]
    attended[...] = values
    normed[...] = norm_rows(values, gain[...][None], shift[...][None]).astype(jnp.bfloat16)


def gelu(values):
    inner = values * (math.sqrt(2 / math.pi) + (math.sqrt(2 / math.pi) * 0.044715) * values * values)
    half = 0.5 * values
    return half + half * jnp.tanh(inner)


def mlp_kernel(inputs, up, bias, down, total):
    hidden = up.shape[0]
    step = 512
    for begin in range(0, hidden, step):
        end = min(begin + step, hidden)
        inner = dot_t(inputs[...], up[begin:end, :]) + bias[begin:end].astype(jnp.float32)[None]
        piece = wide_dot(gelu(inner).astype(jnp.bfloat16), down[begin:end, :])
        if begin == 0:
            total[...] = piece
        else:
            total[...] += piece


def far_mlp_kernel(count, place, inputs, bias, total, *refs):
    ups, downs = refs[:count], refs[count : 2 * count]
    rest = refs[2 * count :]
    rows = ups[0].shape[0]
    hidden = bias.shape[0]
    line = bias[...].astype(jnp.float32)[None]
    parts = [
        line[:, begin : begin + rows]
        for begin in [min(j * rows, hidden - rows) for j in range(count)]
    ]
    bit = 1
    while bit < count:
        turned = (place[0] // bit) % 2 == 1
        parts = [jnp.where(turned, parts[j ^ bit], parts[j]) for j in range(count)]
        bit *= 2
    order = [step ^ core for core in (0, 1) for step in spread_order(count)]
    up, down = rest[-2:]
    for i in range(count):
        up[i * rows : (i + 1) * rows, :] = ups[i][...]
        down[i * rows : (i + 1) * rows, :] = downs[i][...]
    result = total[...]
    group = count // 2
    for half in range(2):
        begin, end = half * group * rows, (half + 1) * group * rows
        shift = jnp.concatenate([parts[j] for j in order[half * group : (half + 1) * group]], 1)
        inner = dot_t(inputs[...], up[begin:end, :]) + shift
        result = result + wide_dot(gelu(inner).astype(jnp.bfloat16), down[begin:end, :])
    if len(rest) > 3:
        attended, last_bias, out = rest[:3]
        out[...] = result + attended[...] + last_bias[...].astype(jnp.float32)[None]
    else:
        rest[0][...] = result.astype(jnp.bfloat16)


def spread_order(holders):
    return [0, holders // 2, 2, holders // 2 + 2]


def run(kernel, room, out_shape, scratch=(), fetched=(), flops=0, scalars=()):
    def call(*args):
        args = list(args)
        specs = []
        buffers = []
        for i, arg in enumerate(args):
            if i in scalars:
                specs.append(pl.BlockSpec(memory_space=pltpu.SMEM))
            elif i in fetched:
                args[i] = pltpu.with_memory_space_constraint(arg, pltpu.HBM)
                specs.append(pl.BlockSpec(memory_space=pltpu.HBM))
                buffers.append(pltpu.VMEM(arg.shape, arg.dtype))
            else:
                specs.append(pl.BlockSpec(memory_space=pltpu.VMEM))

        def body(*refs):
            refs = list(refs)
            if fetched:
                extra = refs[len(refs) - len(buffers) - 1 :]
                refs = refs[: len(refs) - len(buffers) - 1]
                copies = []
                for slot, i in enumerate(fetched):
                    copies.append(
                        pltpu.make_async_copy(refs[i], extra[slot], extra[-1].at[slot])
                    )
                    refs[i] = extra[slot]
                for copy in copies:
                    copy.start()
                for copy in copies:
                    copy.wait()
            kernel(*refs)

        more = buffers + [pltpu.SemaphoreType.DMA((len(buffers),))] if fetched else []
        return pl.pallas_call(
            body,
            in_specs=specs,
            out_shape=out_shape,
            scratch_shapes=list(scratch) + more,
            compiler_params=pltpu.CompilerParams(vmem_limit_bytes=room << 20),
            cost_estimate=pl.CostEstimate(flops=flops, bytes_accessed=0, transcendentals=0),
        )(*args)

    return call


def swapped_layer(sizes):
    seq, dp, tp = sizes

    def per_device(
        patches,
        seg_ids,
        pos_rows,
        pos_cols,
        row_table,
        col_table,
        ln1_gain,
        ln1_bias,
        w_qkv,
        w_out,
        out_bias,
        ln2_gain,
        ln2_bias,
        w_fc1,
        fc1_bias,
        w_fc2,
        fc2_bias,
    ):
        return steps(
            patches,
            seg_ids,
            pos_rows,
            pos_cols,
            row_table,
            col_table,
            ln1_gain,
            ln1_bias,
            w_qkv,
            w_out,
            out_bias,
            ln2_gain,
            ln2_bias,
            w_fc1,
            fc1_bias,
            w_fc2,
            fc2_bias,
        )

    def steps(
        patches,
        seg_ids,
        pos_rows,
        pos_cols,
        row_table,
        col_table,
        ln1_gain,
        ln1_bias,
        w_qkv,
        w_out,
        out_bias,
        ln2_gain,
        ln2_bias,
        w_fc1,
        fc1_bias,
        w_fc2,
        fc2_bias,
    ):
        tokens, width = patches.shape[1:]
        head_dim = width // HEADS
        heads_here = w_qkv.shape[1] // (3 * head_dim)
        hidden = w_fc2.shape[0]
        f32, bf16 = jnp.float32, jnp.bfloat16
        block = (tokens, width)
        sent_block = jax.ShapeDtypeStruct(block, bf16)
        place = lax.axis_index("seq") * dp + lax.axis_index("dp")
        holders = seq * dp
        fc1_rows = w_fc1.T
        qkv_rows = w_qkv.T
        each = 2 * tokens * width

        embedded, normed = run(
            embed_kernel,
            8,
            (pltpu.VMEM(block, f32), sent_block),
            fetched=tuple(range(7)),
            flops=each * 256,
        )(patches[0], pos_rows, pos_cols, row_table, col_table, ln1_gain, ln1_bias)
        normed_other = swap(normed, "seq", seq, 1)
        seg_other = swap(seg_ids, "seq", seq, 1)

        rows = -(-hidden // (8 * holders)) * 8
        overlap = rows * holders - hidden
        begin = jnp.minimum(place * rows, hidden - rows)
        share1 = lax.dynamic_slice(after(fc1_rows, normed), (begin, 0), (rows, width))
        far1 = swap(share1, "tp", tp, 2)
        share2 = lax.dynamic_slice(after(w_fc2, share1), (begin, 0), (rows, width))
        repeated = (place == holders - 1) & (jnp.arange(rows) < overlap)
        share2 = jnp.where(repeated[:, None], jnp.zeros_like(share2), share2)
        far2 = swap(share2, "tp", tp, 2)
        far_bias = swap(fc1_bias, "tp", tp, 2)

        def project(values):
            return run(
                qkv_kernel,
                8,
                pltpu.VMEM((3 * heads_here, head_dim, tokens), bf16),
                flops=each * qkv_rows.shape[0],
            )(values, qkv_rows)

        qkv_own = project(after(normed, share1))
        qkv_other = project(normed_other)

        def spread(share):
            along_x = swap(share, "seq", seq, 1)
            along_y = swap(share, "dp", dp, 2)
            both = swap(share, ("seq", "dp"), seq * dp, dp + 2)
            return [share, along_x, along_y, both]

        def cross(shares):
            return shares + [swap(share, "dp", dp, 1) for share in shares]

        def attend(near, far, seg_near, seg_far, shape):
            scratch = [pltpu.VMEM((heads_here * head_dim, tokens), f32)]
            return run(attend_kernel, 8, shape, scratch, flops=each * 2304)(
                near, far, seg_near, seg_far, w_out
            )

        sent = attend(qkv_other, qkv_own, seg_other, seg_ids, sent_block)
        got = swap(sent, "seq", seq, 1)
        near1 = spread(after(far1, sent))
        kept = attend(
            after(qkv_own, sent, far1, far_bias), qkv_other, seg_ids, seg_other, pltpu.VMEM(block, f32)
        )
        attended, normed2 = run(
            join_kernel, 8, (pltpu.VMEM(block, f32), sent_block), fetched=(3, 4, 5), flops=each * 64
        )(embedded, kept, got, out_bias, ln2_gain, ln2_bias)
        partner = swap(normed2, "tp", tp, 1)
        ups = cross([after(share, normed2) for share in near1])
        near2 = spread(after(far2, normed2))

        def mlp(values):
            return run(
                mlp_kernel, 8, pltpu.VMEM(block, f32), flops=2 * each * hidden
            )(values, fc1_rows, fc1_bias, w_fc2)

        mine = mlp(normed2)
        theirs = mlp(partner)
        downs = cross([after(share, partner) for share in near2])

        def far_mlp(values, total, shape, *tail):
            return run(
                functools.partial(far_mlp_kernel, holders),
                14,
                shape,
                [pltpu.VMEM((holders * rows, width), bf16)] * 2,
                flops=2 * each * hidden,
                scalars=(0,),
            )(place[None], values, far_bias, total, *ups, *downs, *tail)

        back = far_mlp(partner, theirs, sent_block)
        returned = swap(back, "tp", tp, 1)
        ours = far_mlp(after(normed2, back), mine, pltpu.VMEM(block, f32), attended, fc2_bias)
        return (ours + returned.astype(f32)).astype(bf16)[None]

    return per_device


def solution(mesh):
    placed = (
        P(("dp", "tp"), "seq", None),
        P(("dp", "tp"), "seq"),
        P(("dp", "tp"), "seq"),
        P(("dp", "tp"), "seq"),
        P(),
        P(),
        P(),
        P(),
        P(None, "seq"),
        P("seq", None),
        P(),
        P(),
        P(),
        P(None, "tp"),
        P("tp"),
        P("tp", None),
        P(),
    )
    sizes = mesh.shape["seq"], mesh.shape["dp"], mesh.shape["tp"]
    swapped = sizes == (2, 4, 4)
    layer = swapped_layer(sizes) if swapped else gathered_layer
    return jax.shard_map(
        layer,
        mesh=mesh,
        in_specs=placed,
        out_specs=P(("dp", "tp"), "seq", None),
        check_vma=False,
    )
```

```python
import functools
import math

import jax
import jax.numpy as jnp
from jax import lax
from jax.experimental import pallas as pl
from jax.experimental.pallas import tpu as pltpu
from jax.sharding import PartitionSpec as P


HEADS = 16


def layer_norm(values, gain, shift):
    center = jnp.mean(values, -1, keepdims=True)
    spread = jnp.mean(jnp.square(values - center), -1, keepdims=True)
    return (values - center) * lax.rsqrt(spread + 1e-06) * gain + shift


def attend_head(item, segments):
    length = item.shape[0]
    head_dim = item.shape[1] // 3
    block = min(512, length)
    query = item[:, :head_dim].reshape(length // block, block, head_dim)
    seg_query = segments.reshape(length // block, block)
    keys = item[:, head_dim : 2 * head_dim]
    value = item[:, 2 * head_dim :]

    def one_block(pair):
        rows, seg_rows = pair
        scores = lax.dot_general(
            rows, keys, (((1,), (1,)), ((), ())), preferred_element_type=jnp.float32
        ) / math.sqrt(head_dim)
        same = seg_rows[:, None] == segments[None, :]
        scores = jnp.where(same, scores, -jnp.inf)
        top = jnp.max(scores, -1, keepdims=True)
        expo = jnp.exp(scores - top)
        probs = (expo / jnp.sum(expo, -1, keepdims=True)).astype(jnp.bfloat16)
        return jnp.dot(probs, value, preferred_element_type=jnp.float32).astype(jnp.bfloat16)

    return lax.map(one_block, (query, seg_query)).reshape(length, head_dim)


def gathered_layer(
    patches,
    seg_ids,
    pos_rows,
    pos_cols,
    row_table,
    col_table,
    ln1_gain,
    ln1_bias,
    w_qkv,
    w_out,
    out_bias,
    ln2_gain,
    ln2_bias,
    w_fc1,
    fc1_bias,
    w_fc2,
    fc2_bias,
):
    width = patches.shape[2]
    head_dim = width // HEADS
    heads_here = w_qkv.shape[1] // (3 * head_dim)
    levels = jnp.arange(row_table.shape[0], dtype=jnp.int32)
    row_hot = (pos_rows[0][:, None] == levels[None, :]).astype(jnp.bfloat16)
    col_hot = (pos_cols[0][:, None] == levels[None, :]).astype(jnp.bfloat16)
    embedded = patches[0].astype(jnp.float32) + jnp.dot(
        row_hot, row_table, preferred_element_type=jnp.float32
    )
    embedded = embedded + jnp.dot(col_hot, col_table, preferred_element_type=jnp.float32)
    normed = layer_norm(embedded, ln1_gain, ln1_bias).astype(jnp.bfloat16)
    seg_all = lax.all_gather(seg_ids[0], "seq", axis=0, tiled=True)
    qkv = jnp.dot(
        lax.all_gather(normed, "seq", axis=0, tiled=True), w_qkv, preferred_element_type=jnp.float32
    ).astype(jnp.bfloat16)
    mixed = jax.vmap(attend_head, in_axes=(1, None), out_axes=1)(
        qkv.reshape(qkv.shape[0], heads_here, 3 * head_dim), seg_all
    )
    mixed = mixed.reshape(mixed.shape[0], heads_here * head_dim)
    rows = mixed
    projected = lax.psum_scatter(
        jnp.dot(rows, w_out, preferred_element_type=jnp.float32).astype(jnp.bfloat16),
        "seq",
        scatter_dimension=0,
        tiled=True,
    ).astype(jnp.float32)
    attended = embedded + projected + out_bias.astype(jnp.float32)
    normed2 = layer_norm(attended, ln2_gain, ln2_bias).astype(jnp.bfloat16)
    inner = jnp.dot(
        lax.all_gather(normed2, "tp", axis=0, tiled=True), w_fc1, preferred_element_type=jnp.float32
    ) + fc1_bias.astype(jnp.float32)
    hidden = jax.nn.gelu(inner, approximate=True).astype(jnp.bfloat16)
    rows = hidden
    reduced = lax.psum_scatter(
        jnp.dot(rows, w_fc2, preferred_element_type=jnp.float32).astype(jnp.bfloat16),
        "tp",
        scatter_dimension=0,
        tiled=True,
    ).astype(jnp.float32)
    encoded = (attended + reduced + fc2_bias.astype(jnp.float32)).astype(jnp.bfloat16)
    return encoded[None]


def after(value, *earlier):
    return lax.optimization_barrier((value,) + earlier)[0]


def swap(values, axis, size, bit):
    return lax.ppermute(values, axis, [(i, i ^ bit) for i in range(size)])


def wide_dot(left, right):
    return jnp.dot(left, right, preferred_element_type=jnp.float32)


def dot_t(left, right):
    return lax.dot_general(
        left, right, (((1,), (1,)), ((), ())), preferred_element_type=jnp.float32
    )


def tn_dot(left, right):
    return lax.dot_general(
        left, right, (((0,), (0,)), ((), ())), preferred_element_type=jnp.float32
    )


def norm_rows(values, gain, shift):
    center = jnp.mean(values, -1, keepdims=True)
    moved = values - center
    spread = jnp.mean(moved * moved, -1, keepdims=True)
    return moved * lax.rsqrt(spread + 1e-06) * gain + shift


def project_kernel(patch, places, row_tab, col_tab, gain, shift, weight, out, *embedded):
    tokens = patch.shape[0]
    grid = row_tab.shape[0]
    level = lax.broadcasted_iota(jnp.int32, (grid, tokens), 0)
    hot = jnp.concatenate([level == places[0:1, :], level == places[1:2, :]], 0)
    hot = jnp.where(hot, 1.0, 0.0).astype(jnp.bfloat16)
    table = jnp.concatenate([row_tab[...], col_tab[...]], 0)
    values = patch[...].astype(jnp.float32) + tn_dot(hot, table)
    for ref in embedded:
        ref[...] = values
    normed = norm_rows(values, gain[...][None], shift[...][None]).astype(jnp.bfloat16)
    head_dim = out.shape[1]
    product = dot_t(weight[...], normed)
    for part in range(out.shape[0]):
        out[part] = product[part * head_dim : (part + 1) * head_dim].astype(jnp.bfloat16)


def column_of(row):
    length = row.shape[1]
    across = lax.broadcasted_iota(jnp.int32, (length, length), 0)
    along = lax.broadcasted_iota(jnp.int32, (length, length), 1)
    return jnp.sum(jnp.where(across == along, row, 0.0), -1, keepdims=True)


def attend_kernel(near, far, near_places, far_places, weight, out, mixed):
    head_dim = near.shape[1]
    heads = near.shape[0] // 3
    scale = math.log2(math.e) / math.sqrt(head_dim)
    segs = [places[2:3, :].astype(jnp.float32) for places in (near_places, far_places)]
    same = [column_of(seg) == segs[0] for seg in segs]
    for head in range(heads):
        query = near[3 * head]
        scores = []
        for side, keep in zip((near, far), same):
            raw = tn_dot(side[3 * head + 1], query)
            scores.append(jnp.where(keep, raw, -1e30))
        top = jnp.maximum(
            jnp.max(scores[0], 0, keepdims=True), jnp.max(scores[1], 0, keepdims=True)
        )
        total = 0.0
        result = 0.0
        for side, raw in zip((near, far), scores):
            expo = jnp.exp2((raw - top) * scale)
            total = total + jnp.sum(expo, 0, keepdims=True)
            result = result + wide_dot(side[3 * head + 2], expo.astype(jnp.bfloat16))
        mixed[head * head_dim : (head + 1) * head_dim, :] = result / total
    out[...] = tn_dot(mixed[...].astype(jnp.bfloat16), weight[...]).astype(out.dtype)


def join_kernel(embedded, kept, got, bias, gain, shift, attended, normed):
    values = embedded[...] + (kept[...] + got[...].astype(jnp.float32))
    values = values + bias[...].astype(jnp.float32)[None]
    attended[...] = values
    normed[...] = norm_rows(values, gain[...][None], shift[...][None]).astype(jnp.bfloat16)


def gelu(values):
    inner = values * (math.sqrt(2 / math.pi) + (math.sqrt(2 / math.pi) * 0.044715) * values * values)
    half = 0.5 * values
    return half + half * jnp.tanh(inner)


def mlp_kernel(inputs, up, bias, down, total):
    hidden = up.shape[0]
    step = 512
    for begin in range(0, hidden, step):
        end = min(begin + step, hidden)
        inner = dot_t(inputs[...], up[begin:end, :]) + bias[begin:end].astype(jnp.float32)[None]
        piece = wide_dot(gelu(inner).astype(jnp.bfloat16), down[begin:end, :])
        if begin == 0:
            total[...] = piece
        else:
            total[...] += piece


def far_mlp_kernel(count, extra, place, inputs, bias, total, *refs):
    ups, downs = refs[:count], refs[count : 2 * count + extra]
    rest = refs[2 * count + extra :]
    rows = ups[0].shape[0]
    hidden = bias.shape[0]
    line = bias[...].astype(jnp.float32)[None]
    parts = [
        line[:, begin : begin + rows]
        for begin in [min(j * rows, hidden - rows) for j in range(count)]
    ]
    bit = 1
    while bit < count:
        turned = (place[0] // bit) % 2 == 1
        parts = [jnp.where(turned, parts[j ^ bit], parts[j]) for j in range(count)]
        bit *= 2
    order = [step ^ core for core in (0, 1) for step in spread_order(count)]
    up, down = rest[-2:]
    for pieces, whole in ((ups, up), (downs, down)):
        begin = 0
        for piece in pieces:
            whole[begin : begin + piece.shape[0], :] = piece[...]
            begin += piece.shape[0]
    result = total[...]
    group = count // 2
    for half in range(2):
        begin, end = half * group * rows, (half + 1) * group * rows
        shift = jnp.concatenate([parts[j] for j in order[half * group : (half + 1) * group]], 1)
        inner = dot_t(inputs[...], up[begin:end, :]) + shift
        result = result + wide_dot(gelu(inner).astype(jnp.bfloat16), down[begin:end, :])
    if len(rest) > 3:
        attended, last_bias, out = rest[:3]
        out[...] = result + attended[...] + last_bias[...].astype(jnp.float32)[None]
    else:
        rest[0][...] = result.astype(jnp.bfloat16)


def spread_order(holders):
    return [0, holders // 2, 2, holders // 2 + 2]


def run(kernel, room, out_shape, scratch=(), fetched=(), flops=0, scalars=()):
    def call(*args):
        args = list(args)
        specs = []
        buffers = []
        for i, arg in enumerate(args):
            if i in scalars:
                specs.append(pl.BlockSpec(memory_space=pltpu.SMEM))
            elif i in fetched:
                args[i] = pltpu.with_memory_space_constraint(arg, pltpu.HBM)
                specs.append(pl.BlockSpec(memory_space=pltpu.HBM))
                buffers.append(pltpu.VMEM(arg.shape, arg.dtype))
            else:
                specs.append(pl.BlockSpec(memory_space=pltpu.VMEM))

        def body(*refs):
            refs = list(refs)
            if fetched:
                extra = refs[len(refs) - len(buffers) - 1 :]
                refs = refs[: len(refs) - len(buffers) - 1]
                copies = []
                for slot, i in enumerate(fetched):
                    copies.append(
                        pltpu.make_async_copy(refs[i], extra[slot], extra[-1].at[slot])
                    )
                    refs[i] = extra[slot]
                for copy in copies:
                    copy.start()
                for copy in copies:
                    copy.wait()
            kernel(*refs)

        more = buffers + [pltpu.SemaphoreType.DMA((len(buffers),))] if fetched else []
        return pl.pallas_call(
            body,
            in_specs=specs,
            out_shape=out_shape,
            scratch_shapes=list(scratch) + more,
            compiler_params=pltpu.CompilerParams(vmem_limit_bytes=room << 20),
            cost_estimate=pl.CostEstimate(flops=flops, bytes_accessed=0, transcendentals=0),
        )(*args)

    return call


def swapped_layer(sizes):
    seq, dp, tp = sizes

    def per_device(
        patches,
        seg_ids,
        pos_rows,
        pos_cols,
        row_table,
        col_table,
        ln1_gain,
        ln1_bias,
        w_qkv,
        w_out,
        out_bias,
        ln2_gain,
        ln2_bias,
        w_fc1,
        fc1_bias,
        w_fc2,
        fc2_bias,
    ):
        return steps(
            patches,
            seg_ids,
            pos_rows,
            pos_cols,
            row_table,
            col_table,
            ln1_gain,
            ln1_bias,
            w_qkv,
            w_out,
            out_bias,
            ln2_gain,
            ln2_bias,
            w_fc1,
            fc1_bias,
            w_fc2,
            fc2_bias,
        )

    def steps(
        patches,
        seg_ids,
        pos_rows,
        pos_cols,
        row_table,
        col_table,
        ln1_gain,
        ln1_bias,
        w_qkv,
        w_out,
        out_bias,
        ln2_gain,
        ln2_bias,
        w_fc1,
        fc1_bias,
        w_fc2,
        fc2_bias,
    ):
        tokens, width = patches.shape[1:]
        head_dim = width // HEADS
        heads_here = w_qkv.shape[1] // (3 * head_dim)
        hidden = w_fc2.shape[0]
        f32, bf16 = jnp.float32, jnp.bfloat16
        block = (tokens, width)
        sent_block = jax.ShapeDtypeStruct(block, bf16)
        place = lax.axis_index("seq") * dp + lax.axis_index("dp")
        holders = seq * dp
        fc1_rows = w_fc1.T
        qkv_rows = w_qkv.T
        each = 2 * tokens * width

        places = jnp.concatenate([pos_rows, pos_cols, seg_ids])
        patches_other = swap(patches[0], "seq", seq, 1)
        places_other = swap(places, "seq", seq, 1)

        rows = -(-hidden // (8 * holders)) * 8
        overlap = rows * holders - hidden
        begin = jnp.minimum(place * rows, hidden - rows)
        share1 = lax.dynamic_slice(fc1_rows, (begin, 0), (rows, width))
        far1 = swap(share1, "tp", tp, 2)
        far_bias = swap(fc1_bias, "tp", tp, 2)

        def project(values, where, fetched, *more):
            qkv_shape = pltpu.VMEM((3 * heads_here, head_dim, tokens), bf16)
            return run(
                project_kernel,
                8,
                (qkv_shape,) + more,
                fetched=fetched,
                flops=each * (qkv_rows.shape[0] + 256),
            )(values, where, row_table, col_table, ln1_gain, ln1_bias, qkv_rows)

        qkv_own, embedded = project(
            after(patches[0], share1), places, (0, 2, 3, 4, 5), pltpu.VMEM(block, f32)
        )
        share2 = lax.dynamic_slice(after(w_fc2, share1), (begin, 0), (rows, width))
        repeated = (place == holders - 1) & (jnp.arange(rows) < overlap)
        share2 = jnp.where(repeated[:, None], jnp.zeros_like(share2), share2)
        (qkv_other,) = project(after(patches_other, qkv_own, share2), places_other, ())

        def spread(share):
            along_x = swap(share, "seq", seq, 1)
            along_y = swap(share, "dp", dp, 2)
            return [share, along_x, along_y]

        def cross(shares):
            return shares + [swap(share, "dp", dp, 1) for share in shares]

        def attend(near, far, near_places, far_places, shape):
            scratch = [pltpu.VMEM((heads_here * head_dim, tokens), f32)]
            return run(attend_kernel, 8, shape, scratch, flops=each * 2304)(
                near, far, near_places, far_places, w_out
            )

        sent = attend(qkv_other, qkv_own, places_other, places, sent_block)
        got = swap(sent, "seq", seq, 1)
        far2 = swap(after(share2, sent), "tp", tp, 2)
        near1 = spread(after(far1, sent))
        kept = attend(after(qkv_own, sent), qkv_other, places, places_other, pltpu.VMEM(block, f32))
        attended, normed2 = run(
            join_kernel, 8, (pltpu.VMEM(block, f32), sent_block), fetched=(3, 4, 5), flops=each * 64
        )(embedded, kept, got, out_bias, ln2_gain, ln2_bias)
        partner = swap(normed2, "tp", tp, 1)
        near1 = near1 + [swap(after(near1[1], normed2), "dp", dp, 2)]
        ups = cross([after(share, normed2) for share in near1])
        near2 = spread(after(far2, normed2))
        near2 = near2 + [swap(near2[2], "seq", seq, 1)]

        def mlp(values):
            return run(
                mlp_kernel, 8, pltpu.VMEM(block, f32), flops=2 * each * hidden
            )(values, fc1_rows, fc1_bias, w_fc2)

        mine = mlp(normed2)
        theirs = mlp(partner)
        downs = cross([after(share, partner) for share in near2])

        def far_mlp(values, total, shape, *tail):
            return run(
                functools.partial(far_mlp_kernel, holders, len(downs) - holders),
                14,
                shape,
                [pltpu.VMEM((holders * rows, width), bf16)] * 2,
                flops=2 * each * hidden,
                scalars=(0,),
            )(place[None], values, far_bias, total, *ups, *downs, *tail)

        back = far_mlp(partner, theirs, sent_block)
        returned = swap(back, "tp", tp, 1)
        ours = far_mlp(after(normed2, back), mine, pltpu.VMEM(block, f32), attended, fc2_bias)
        return (ours + returned.astype(f32)).astype(bf16)[None]

    return per_device


def solution(mesh):
    placed = (
        P(("dp", "tp"), "seq", None),
        P(("dp", "tp"), "seq"),
        P(("dp", "tp"), "seq"),
        P(("dp", "tp"), "seq"),
        P(),
        P(),
        P(),
        P(),
        P(None, "seq"),
        P("seq", None),
        P(),
        P(),
        P(),
        P(None, "tp"),
        P("tp"),
        P("tp", None),
        P(),
    )
    sizes = mesh.shape["seq"], mesh.shape["dp"], mesh.shape["tp"]
    swapped = sizes == (2, 4, 4)
    layer = swapped_layer(sizes) if swapped else gathered_layer
    return jax.shard_map(
        layer,
        mesh=mesh,
        in_specs=placed,
        out_specs=P(("dp", "tp"), "seq", None),
        check_vma=False,
    )
```

```python
import functools
import math

import jax
import jax.numpy as jnp
from jax import lax
from jax.experimental import pallas as pl
from jax.experimental.pallas import tpu as pltpu
from jax.sharding import PartitionSpec as P


HEADS = 16


def layer_norm(values, gain, shift):
    center = jnp.mean(values, -1, keepdims=True)
    spread = jnp.mean(jnp.square(values - center), -1, keepdims=True)
    return (values - center) * lax.rsqrt(spread + 1e-06) * gain + shift


def attend_head(item, segments):
    length = item.shape[0]
    head_dim = item.shape[1] // 3
    block = min(512, length)
    query = item[:, :head_dim].reshape(length // block, block, head_dim)
    seg_query = segments.reshape(length // block, block)
    keys = item[:, head_dim : 2 * head_dim]
    value = item[:, 2 * head_dim :]

    def one_block(pair):
        rows, seg_rows = pair
        scores = lax.dot_general(
            rows, keys, (((1,), (1,)), ((), ())), preferred_element_type=jnp.float32
        ) / math.sqrt(head_dim)
        same = seg_rows[:, None] == segments[None, :]
        scores = jnp.where(same, scores, -jnp.inf)
        top = jnp.max(scores, -1, keepdims=True)
        expo = jnp.exp(scores - top)
        probs = (expo / jnp.sum(expo, -1, keepdims=True)).astype(jnp.bfloat16)
        return jnp.dot(probs, value, preferred_element_type=jnp.float32).astype(jnp.bfloat16)

    return lax.map(one_block, (query, seg_query)).reshape(length, head_dim)


def gathered_layer(
    patches,
    seg_ids,
    pos_rows,
    pos_cols,
    row_table,
    col_table,
    ln1_gain,
    ln1_bias,
    w_qkv,
    w_out,
    out_bias,
    ln2_gain,
    ln2_bias,
    w_fc1,
    fc1_bias,
    w_fc2,
    fc2_bias,
):
    width = patches.shape[2]
    head_dim = width // HEADS
    heads_here = w_qkv.shape[1] // (3 * head_dim)
    levels = jnp.arange(row_table.shape[0], dtype=jnp.int32)
    row_hot = (pos_rows[0][:, None] == levels[None, :]).astype(jnp.bfloat16)
    col_hot = (pos_cols[0][:, None] == levels[None, :]).astype(jnp.bfloat16)
    embedded = patches[0].astype(jnp.float32) + jnp.dot(
        row_hot, row_table, preferred_element_type=jnp.float32
    )
    embedded = embedded + jnp.dot(col_hot, col_table, preferred_element_type=jnp.float32)
    normed = layer_norm(embedded, ln1_gain, ln1_bias).astype(jnp.bfloat16)
    seg_all = lax.all_gather(seg_ids[0], "seq", axis=0, tiled=True)
    qkv = jnp.dot(
        lax.all_gather(normed, "seq", axis=0, tiled=True), w_qkv, preferred_element_type=jnp.float32
    ).astype(jnp.bfloat16)
    mixed = jax.vmap(attend_head, in_axes=(1, None), out_axes=1)(
        qkv.reshape(qkv.shape[0], heads_here, 3 * head_dim), seg_all
    )
    mixed = mixed.reshape(mixed.shape[0], heads_here * head_dim)
    rows = mixed
    projected = lax.psum_scatter(
        jnp.dot(rows, w_out, preferred_element_type=jnp.float32).astype(jnp.bfloat16),
        "seq",
        scatter_dimension=0,
        tiled=True,
    ).astype(jnp.float32)
    attended = embedded + projected + out_bias.astype(jnp.float32)
    normed2 = layer_norm(attended, ln2_gain, ln2_bias).astype(jnp.bfloat16)
    inner = jnp.dot(
        lax.all_gather(normed2, "tp", axis=0, tiled=True), w_fc1, preferred_element_type=jnp.float32
    ) + fc1_bias.astype(jnp.float32)
    hidden = jax.nn.gelu(inner, approximate=True).astype(jnp.bfloat16)
    rows = hidden
    reduced = lax.psum_scatter(
        jnp.dot(rows, w_fc2, preferred_element_type=jnp.float32).astype(jnp.bfloat16),
        "tp",
        scatter_dimension=0,
        tiled=True,
    ).astype(jnp.float32)
    encoded = (attended + reduced + fc2_bias.astype(jnp.float32)).astype(jnp.bfloat16)
    return encoded[None]


def after(value, *earlier):
    return lax.optimization_barrier((value,) + earlier)[0]


def swap(values, axis, size, bit):
    return lax.ppermute(values, axis, [(i, i ^ bit) for i in range(size)])


def wide_dot(left, right):
    return jnp.dot(left, right, preferred_element_type=jnp.float32)


def dot_t(left, right):
    return lax.dot_general(
        left, right, (((1,), (1,)), ((), ())), preferred_element_type=jnp.float32
    )


def tn_dot(left, right):
    return lax.dot_general(
        left, right, (((0,), (0,)), ((), ())), preferred_element_type=jnp.float32
    )


def norm_rows(values, gain, shift):
    center = jnp.mean(values, -1, keepdims=True)
    moved = values - center
    spread = jnp.mean(moved * moved, -1, keepdims=True)
    return moved * lax.rsqrt(spread + 1e-06) * gain + shift


def project_kernel(
    patch, places, row_tab, col_tab, gain, shift, weight, out, *embedded, arrive=None
):
    tokens = patch.shape[0]
    grid = row_tab.shape[0]
    level = lax.broadcasted_iota(jnp.int32, (grid, tokens), 0)
    hot = jnp.concatenate([level == places[0:1, :], level == places[1:2, :]], 0)
    hot = jnp.where(hot, 1.0, 0.0).astype(jnp.bfloat16)
    table = jnp.concatenate([row_tab[...], col_tab[...]], 0)
    values = patch[...].astype(jnp.float32) + tn_dot(hot, table)
    for ref in embedded:
        ref[...] = values
    normed = norm_rows(values, gain[...][None], shift[...][None]).astype(jnp.bfloat16)
    head_dim = out.shape[1]
    if arrive:
        arrive()
    product = dot_t(weight[...], normed)
    for part in range(out.shape[0]):
        out[part] = product[part * head_dim : (part + 1) * head_dim].astype(jnp.bfloat16)


def column_of(row):
    length = row.shape[1]
    across = lax.broadcasted_iota(jnp.int32, (length, length), 0)
    along = lax.broadcasted_iota(jnp.int32, (length, length), 1)
    return jnp.sum(jnp.where(across == along, row, 0.0), -1, keepdims=True)


def attend_kernel(near, far, near_places, far_places, weight, out, mixed, scores, probs):
    head_dim = near.shape[1]
    heads = near.shape[0] // 3
    scale = math.log2(math.e) / math.sqrt(head_dim)
    segs = [places[2:3, :].astype(jnp.float32) for places in (near_places, far_places)]
    bias = [jnp.where(column_of(seg) == segs[0], 0.0, -1e30) for seg in segs]
    tokens = near.shape[2]
    for head in range(heads):
        query = near[3 * head]
        for i, side in enumerate((near, far)):
            raw = tn_dot(side[3 * head + 1], query)
            scores[head, i * tokens : (i + 1) * tokens, :] = raw + bias[i]
    shares = []
    for head in range(heads):
        raw = scores[head]
        expo = jnp.exp2((raw - jnp.max(raw, 0, keepdims=True)) * scale)
        shares.append(1.0 / jnp.sum(expo, 0, keepdims=True))
        probs[head] = expo.astype(jnp.bfloat16)
    for head in range(heads):
        result = wide_dot(near[3 * head + 2], probs[head, :tokens, :])
        result = result + wide_dot(far[3 * head + 2], probs[head, tokens:, :])
        mixed[head * head_dim : (head + 1) * head_dim, :] = result * shares[head]
    out[...] = tn_dot(mixed[...].astype(jnp.bfloat16), weight[...]).astype(out.dtype)


def join_kernel(embedded, kept, got, bias, gain, shift, attended, normed):
    values = embedded[...] + (kept[...] + got[...].astype(jnp.float32))
    values = values + bias[...].astype(jnp.float32)[None]
    attended[...] = values
    normed[...] = norm_rows(values, gain[...][None], shift[...][None]).astype(jnp.bfloat16)


def gelu(values):
    inner = values * (math.sqrt(2 / math.pi) + (math.sqrt(2 / math.pi) * 0.044715) * values * values)
    half = 0.5 * values
    return half + half * jnp.tanh(inner)


def mlp_kernel(inputs, up, bias, down, total):
    hidden = up.shape[0]
    step = 512
    for begin in range(0, hidden, step):
        end = min(begin + step, hidden)
        inner = dot_t(inputs[...], up[begin:end, :]) + bias[begin:end].astype(jnp.float32)[None]
        piece = wide_dot(gelu(inner).astype(jnp.bfloat16), down[begin:end, :])
        if begin == 0:
            total[...] = piece
        else:
            total[...] += piece


def far_mlp_kernel(count, picks, place, inputs, bias, total, *refs):
    ups, downs = refs[: len(picks)], refs[len(picks) : 2 * len(picks)]
    rest = refs[2 * len(picks) :]
    rows = ups[0].shape[0]
    hidden = bias.shape[0]
    line = bias[...].astype(jnp.float32)[None]
    parts = [
        line[:, begin : begin + rows]
        for begin in [min(j * rows, hidden - rows) for j in range(count)]
    ]
    bit = 1
    while bit < count:
        turned = (place[0] // bit) % 2 == 1
        parts = [jnp.where(turned, parts[j ^ bit], parts[j]) for j in range(count)]
        bit *= 2
    order = [step ^ core for core in (0, 1) for step in spread_order(count)]
    up, down = rest[-2:]
    for i in range(len(picks)):
        up[i * rows : (i + 1) * rows, :] = ups[i][...]
        down[i * rows : (i + 1) * rows, :] = downs[i][...]
    result = total[...]
    group = len(picks) // 2 if len(picks) == count else len(picks)
    for first in range(0, len(picks), group):
        begin, end = first * rows, (first + group) * rows
        shift = jnp.concatenate([parts[order[p]] for p in picks[first : first + group]], 1)
        inner = dot_t(inputs[...], up[begin:end, :]) + shift
        result = result + wide_dot(gelu(inner).astype(jnp.bfloat16), down[begin:end, :])
    if len(rest) > 3:
        attended, last_bias, out = rest[:3]
        out[...] = result + attended[...] + last_bias[...].astype(jnp.float32)[None]
    else:
        rest[0][...] = result.astype(rest[0].dtype)


def spread_order(holders):
    return [0, holders // 2, 2, holders // 2 + 2]


def run(kernel, room, out_shape, scratch=(), fetched=(), late=(), flops=0, scalars=()):
    def call(*args):
        args = list(args)
        specs = []
        buffers = []
        for i, arg in enumerate(args):
            if i in scalars:
                specs.append(pl.BlockSpec(memory_space=pltpu.SMEM))
            elif i in fetched:
                args[i] = pltpu.with_memory_space_constraint(arg, pltpu.HBM)
                specs.append(pl.BlockSpec(memory_space=pltpu.HBM))
                buffers.append(pltpu.VMEM(arg.shape, arg.dtype))
            else:
                specs.append(pl.BlockSpec(memory_space=pltpu.VMEM))

        def body(*refs):
            refs = list(refs)
            if fetched:
                extra = refs[len(refs) - len(buffers) - 1 :]
                refs = refs[: len(refs) - len(buffers) - 1]
                copies = []
                for slot, i in enumerate(fetched):
                    copies.append(
                        pltpu.make_async_copy(refs[i], extra[slot], extra[-1].at[slot])
                    )
                    refs[i] = extra[slot]
                for copy in copies:
                    copy.start()
                for slot, i in enumerate(fetched):
                    if i not in late:
                        copies[slot].wait()

                def arrive():
                    for slot, i in enumerate(fetched):
                        if i in late:
                            copies[slot].wait()

                if late:
                    kernel(*refs, arrive=arrive)
                    return
            kernel(*refs)

        more = buffers + [pltpu.SemaphoreType.DMA((len(buffers),))] if fetched else []
        return pl.pallas_call(
            body,
            in_specs=specs,
            out_shape=out_shape,
            scratch_shapes=list(scratch) + more,
            compiler_params=pltpu.CompilerParams(vmem_limit_bytes=room << 20),
            cost_estimate=pl.CostEstimate(flops=flops, bytes_accessed=0, transcendentals=0),
        )(*args)

    return call


def swapped_layer(sizes):
    seq, dp, tp = sizes

    def per_device(
        patches,
        seg_ids,
        pos_rows,
        pos_cols,
        row_table,
        col_table,
        ln1_gain,
        ln1_bias,
        w_qkv,
        w_out,
        out_bias,
        ln2_gain,
        ln2_bias,
        w_fc1,
        fc1_bias,
        w_fc2,
        fc2_bias,
    ):
        return steps(
            patches,
            seg_ids,
            pos_rows,
            pos_cols,
            row_table,
            col_table,
            ln1_gain,
            ln1_bias,
            w_qkv,
            w_out,
            out_bias,
            ln2_gain,
            ln2_bias,
            w_fc1,
            fc1_bias,
            w_fc2,
            fc2_bias,
        )

    def steps(
        patches,
        seg_ids,
        pos_rows,
        pos_cols,
        row_table,
        col_table,
        ln1_gain,
        ln1_bias,
        w_qkv,
        w_out,
        out_bias,
        ln2_gain,
        ln2_bias,
        w_fc1,
        fc1_bias,
        w_fc2,
        fc2_bias,
    ):
        tokens, width = patches.shape[1:]
        head_dim = width // HEADS
        heads_here = w_qkv.shape[1] // (3 * head_dim)
        hidden = w_fc2.shape[0]
        f32, bf16 = jnp.float32, jnp.bfloat16
        block = (tokens, width)
        sent_block = jax.ShapeDtypeStruct(block, bf16)
        place = lax.axis_index("seq") * dp + lax.axis_index("dp")
        holders = seq * dp
        fc1_rows = w_fc1.T
        qkv_rows = w_qkv.T
        each = 2 * tokens * width

        places = jnp.concatenate([pos_rows, pos_cols, seg_ids])
        patches_other = swap(patches[0], "seq", seq, 1)
        places_other = swap(places, "seq", seq, 1)

        rows = -(-hidden // (8 * holders)) * 8
        overlap = rows * holders - hidden
        begin = jnp.minimum(place * rows, hidden - rows)
        share1 = lax.dynamic_slice(fc1_rows, (begin, 0), (rows, width))
        far1 = swap(share1, "tp", tp, 2)
        far_bias = swap(fc1_bias, "tp", tp, 2)

        def project(values, where, fetched, *more):
            qkv_shape = pltpu.VMEM((3 * heads_here, head_dim, tokens), bf16)
            return run(
                project_kernel,
                14,
                (qkv_shape,) + more,
                fetched=fetched,
                late=(6,) if fetched else (),
                flops=each * (qkv_rows.shape[0] + 256),
            )(values, where, row_table, col_table, ln1_gain, ln1_bias, qkv_rows)

        qkv_own, embedded = project(
            after(patches[0], share1), places, (0, 2, 3, 4, 5, 6), pltpu.VMEM(block, f32)
        )
        share2 = lax.dynamic_slice(after(w_fc2, share1), (begin, 0), (rows, width))
        repeated = (place == holders - 1) & (jnp.arange(rows) < overlap)
        share2 = jnp.where(repeated[:, None], jnp.zeros_like(share2), share2)
        (qkv_other,) = project(after(patches_other, qkv_own, share2), places_other, ())

        def spread(share):
            along_x = swap(share, "seq", seq, 1)
            along_y = swap(share, "dp", dp, 2)
            return [share, along_x, along_y]

        def cross(shares):
            return shares + [swap(share, "dp", dp, 1) for share in shares]

        def attend(near, far, near_places, far_places, shape):
            scratch = [
                pltpu.VMEM((heads_here * head_dim, tokens), f32),
                pltpu.VMEM((heads_here, 2 * tokens, tokens), f32),
                pltpu.VMEM((heads_here, 2 * tokens, tokens), bf16),
            ]
            return run(attend_kernel, 14, shape, scratch, flops=each * 2304)(
                near, far, near_places, far_places, w_out
            )

        sent = attend(qkv_other, qkv_own, places_other, places, sent_block)
        far2 = swap(after(share2, sent), "tp", tp, 2)
        got = swap(sent, "seq", seq, 1)
        near1 = spread(after(far1, sent))
        kept = attend(after(qkv_own, sent), qkv_other, places, places_other, pltpu.VMEM(block, f32))
        attended, normed2 = run(
            join_kernel, 8, (pltpu.VMEM(block, f32), sent_block), fetched=(3, 4, 5), flops=each * 64
        )(embedded, kept, got, out_bias, ln2_gain, ln2_bias)
        partner = swap(normed2, "tp", tp, 1)
        near1 = near1 + [swap(after(near1[1], normed2), "dp", dp, 2)]
        ups = cross([after(share, normed2) for share in near1])
        near2 = spread(after(far2, normed2))
        near2 = near2 + [swap(near2[2], "seq", seq, 1)]

        def mlp(values):
            return run(
                mlp_kernel, 8, pltpu.VMEM(block, f32), flops=2 * each * hidden
            )(values, fc1_rows, fc1_bias, w_fc2)

        mine = mlp(normed2)
        theirs = mlp(partner)
        downs = cross([after(share, partner) for share in near2])

        def far_mlp(picks, values, total, shape, *tail):
            pieces = [ups[p] for p in picks] + [downs[p] for p in picks]
            return run(
                functools.partial(far_mlp_kernel, holders, picks),
                14,
                shape,
                [pltpu.VMEM((len(picks) * rows, width), bf16)] * 2,
                flops=2 * each * len(picks) * rows,
                scalars=(0,),
            )(place[None], values, far_bias, total, *pieces, *tail)

        late = (holders // 2 - 1, holders - 1)
        soon = tuple(p for p in range(holders) if p not in late)
        theirs = far_mlp(soon, partner, theirs, pltpu.VMEM(block, f32))
        back = far_mlp(late, partner, theirs, sent_block)
        returned = swap(back, "tp", tp, 1)
        ours = far_mlp(
            tuple(range(holders)),
            after(normed2, back),
            mine,
            pltpu.VMEM(block, f32),
            attended,
            fc2_bias,
        )
        return (ours + returned.astype(f32)).astype(bf16)[None]

    return per_device


def solution(mesh):
    placed = (
        P(("dp", "tp"), "seq", None),
        P(("dp", "tp"), "seq"),
        P(("dp", "tp"), "seq"),
        P(("dp", "tp"), "seq"),
        P(),
        P(),
        P(),
        P(),
        P(None, "seq"),
        P("seq", None),
        P(),
        P(),
        P(),
        P(None, "tp"),
        P("tp"),
        P("tp", None),
        P(),
    )
    sizes = mesh.shape["seq"], mesh.shape["dp"], mesh.shape["tp"]
    swapped = sizes == (2, 4, 4)
    layer = swapped_layer(sizes) if swapped else gathered_layer
    return jax.shard_map(
        layer,
        mesh=mesh,
        in_specs=placed,
        out_specs=P(("dp", "tp"), "seq", None),
        check_vma=False,
    )
```
